256 devices in a mesh: dp: 32 (over z, y), mp: 8 (over x, core).
Axes of the slice: x: 4, y: 4, z: 8, core: 2. Of those that a mesh axis runs over, the one named last changes fastest.
Arguments:
- queries: bfloat16 [4096, 8192], P('dp', 'mp'), may hold values from -8 to 8
- tree_keys: bfloat16 [4096, 1024], P('dp', 'mp'), may hold values from -18 to 18
- tree_values: bfloat16 [4096, 1024], P('dp', 'mp'), may hold values from -6 to 6
- cache_keys: bfloat16 [64, 4096, 1024], P('dp', None, 'mp'), may hold values from -8 to 8
- cache_values: bfloat16 [64, 4096, 1024], P('dp', None, 'mp'), may hold values from -6 to 6
- cache_lens: int32 [64], P('dp'), may hold values from 1024 to 4096, as said below
- parents: int32 [64, 64], P('dp'), may hold values from -1 to 62, as said below
- accepted_nodes: int32 [64, 8], P('dp'), may hold values from 0 to 63, as said below
- residual: bfloat16 [4096, 8192], P('dp', 'mp'), may hold values from -1.796875 to 1.796875
- out_weight: bfloat16 [8192, 8192], P('mp', 'dp'), may hold values from -0.0625 to 0.0625
Outputs:
- tree_hidden: bfloat16 [4096, 8192], P('dp', 'mp')
- accepted_hidden: bfloat16 [512, 8192], P(None, 'mp')
The draws below stay inside these ranges and needn't reach their ends.
Inputs may be any that keep to these rules, and one draw needn't show every extreme that they name: parents[r, 0] = -1 and 0 <= parents[r, i] < i for i >= 1. accepted_nodes[r, 0] = 0, the nodes of a row increase, and parents[r, accepted_nodes[r, a + 1]] = accepted_nodes[r, a]. `cache_lens`: some request has exactly 4096 filled positions.
All inputs are finite; a program needn't handle non-finite values.
Results may differ from the reference program's by a relative error of at most 0.015.
Values may be sent and summed in bfloat16 or wider, within the bound.
No kernel may reach another device: no remote copies, remote signals or barrier semaphores. Data moves between devices by JAX's collectives and lax.ppermute only.
A program may use at most 64 MiB of HBM per device.

```python
import math
import jax
import jax.numpy as jnp
from jax import lax

D = 8192
HEADS = 64
KV_HEADS = 8
HD = 128
NODES = 64
ACC = 8
CACHE = 4096
REQUESTS = 64
ROWS = 4096


def tree_shape(key):

    def one_tree(tree_key):
        chain_key, parent_key = jax.random.split(tree_key)
        shuffled = jax.random.permutation(chain_key, NODES - 1) + 1
        chain_nodes = jnp.sort(shuffled[:ACC - 1]).astype(jnp.int32)
        positions = jnp.arange(NODES, dtype=jnp.int32)
        parent_list = jax.random.randint(parent_key, (NODES,), 0, jnp.maximum(positions, 1)).astype(jnp.int32)
        parent_list = jnp.where(positions == 0, -1, parent_list)
        previous = jnp.concatenate([jnp.zeros((1,), jnp.int32), chain_nodes[:-1]])
        parent_list = parent_list.at[chain_nodes].set(previous)
        accepted = jnp.concatenate([jnp.zeros((1,), jnp.int32), chain_nodes])
        return (parent_list, accepted)
    request_keys = jax.random.split(jax.random.fold_in(key, 11), REQUESTS)
    return jax.vmap(one_tree)(request_keys)


def draw_parents(key, part):
    return tree_shape(key)[0].astype(jnp.int32)


def draw_accepted_nodes(key, part):
    return tree_shape(key)[1].astype(jnp.int32)


def draw_cache_lens(key, part):
    length_key, chosen_key = jax.random.split(jax.random.fold_in(key, 31))
    lengths = jax.random.randint(length_key, (REQUESTS,), CACHE // 4, CACHE + 1)
    chosen = jax.random.randint(chosen_key, (), 0, REQUESTS)
    return jnp.where(jnp.arange(REQUESTS) == chosen, CACHE, lengths).astype(jnp.int32)


def draw_cache_keys(key, part):
    shape = (REQUESTS, CACHE, KV_HEADS * HD)
    values = jax.random.normal(jax.random.fold_in(key, 1), shape, jnp.float32)
    return jnp.clip(values, -8.0, 8.0).astype(jnp.bfloat16)


def draw_queries(key, part):
    shape = (REQUESTS * NODES, HEADS * HD)
    values = 1.7 * jax.random.normal(jax.random.fold_in(key, 3), shape, jnp.float32)
    return jnp.clip(values, -8.0, 8.0).astype(jnp.bfloat16)


def block_levels(rng, extent, shards, low, top_value):
    def one(position, shards_of):
        draws = jax.random.uniform(jax.random.fold_in(jax.random.fold_in(rng, 6), position), (shards_of,), jnp.float32, low / len(shards), top_value / len(shards))
        return jnp.repeat(jnp.exp(draws), extent[position] // shards_of).reshape((-1,) + (1,) * (len(extent) - position - 1))

    loudness = one(*shards[0])
    for cut in shards[1:]:
        loudness = loudness * one(*cut)
    return loudness


def normal_values(stream_key, dims, deviation, reach, shards=(), kind=jnp.bfloat16):
    result = deviation * jax.random.normal(stream_key, dims, jnp.float32)
    if shards:
        result = result * block_levels(stream_key, dims, shards, -0.22, 0.18)
    return jnp.clip(result, -reach, reach).astype(kind)


def setup_inputs(seed: int = 0) -> dict:
    key_list = jax.random.split(jax.random.key(seed), 11)
    return {
        "queries": draw_queries(jax.random.fold_in(key_list[10], 71), 0),
        "tree_keys": normal_values(key_list[1], (ROWS, KV_HEADS * HD), 3.0, 18.0, ((0, 32), (1, 8))),
        "tree_values": normal_values(key_list[2], (ROWS, KV_HEADS * HD), 1.0, 6.0, ((0, 32), (1, 8))),
        "cache_keys": draw_cache_keys(jax.random.fold_in(key_list[10], 71), 0),
        "cache_values": normal_values(key_list[4], (REQUESTS, CACHE, KV_HEADS * HD), 1.0, 6.0, ((0, 32), (2, 8))),
        "cache_lens": draw_cache_lens(jax.random.fold_in(key_list[10], 71), 0),
        "parents": draw_parents(jax.random.fold_in(key_list[10], 71), 0),
        "accepted_nodes": draw_accepted_nodes(jax.random.fold_in(key_list[10], 71), 0),
        "residual": normal_values(key_list[8], (ROWS, D), 0.3, 1.796875, ((0, 32), (1, 8))),
        "out_weight": normal_values(key_list[9], (HEADS * HD, D), (HEADS * HD) ** -0.5, 0.0625, ((0, 8), (1, 32))),
    }


neg_large = -1e+30

def ancestry(parents):
    positions = jnp.arange(NODES, dtype=jnp.int32)
    parent_hot = (parents[:, :, None] == positions[None, None, :]).astype(jnp.float32)
    reached = parent_hot + jnp.eye(NODES, dtype=jnp.float32)[None]
    for squaring in range((NODES - 1).bit_length()):
        reached = jnp.minimum(jnp.einsum('rij,rjk->rik', reached, reached, precision=lax.Precision.HIGHEST), 1.0)
    return reached > 0.5

def reference(queries, tree_keys, tree_values, cache_keys, cache_values, cache_lens, parents, accepted_nodes, residual, out_weight):
    group_size = HEADS // KV_HEADS
    scale_factor = 1.0 / math.sqrt(HD)
    ancestor = ancestry(parents)
    query_grid = queries.reshape(REQUESTS, NODES, KV_HEADS, group_size, HD)
    tree_key_grid = tree_keys.reshape(REQUESTS, NODES, KV_HEADS, HD)
    tree_value_grid = tree_values.reshape(REQUESTS, NODES, KV_HEADS, HD)
    cache_key_grid = cache_keys.reshape(REQUESTS, CACHE, KV_HEADS, HD)
    cache_value_grid = cache_values.reshape(REQUESTS, CACHE, KV_HEADS, HD)

    def one_request(request_data):
        query_one, tkey_one, tvalue_one, ckey_one, cvalue_one, cache_length, mask_one = request_data
        query_float = query_one.astype(jnp.float32)
        cache_scores = jnp.einsum('nkgd,pkd->nkgp', query_float, ckey_one.astype(jnp.float32), precision=lax.Precision.HIGHEST) * scale_factor
        live_keys = jnp.arange(CACHE, dtype=jnp.int32) < cache_length
        cache_scores = jnp.where(live_keys[None, None, None, :], cache_scores, neg_large)
        tree_scores = jnp.einsum('nkgd,jkd->nkgj', query_float, tkey_one.astype(jnp.float32), precision=lax.Precision.HIGHEST) * scale_factor
        tree_scores = jnp.where(mask_one[:, None, None, :], tree_scores, neg_large)
        row_max = jnp.maximum(lax.optimization_barrier(jnp.max(cache_scores, axis=-1)), lax.optimization_barrier(jnp.max(tree_scores, axis=-1)))
        cache_weights = jnp.exp(cache_scores - row_max[..., None])
        tree_weights = jnp.exp(tree_scores - row_max[..., None])
        denominator = lax.optimization_barrier(jnp.sum(cache_weights, axis=-1)) + lax.optimization_barrier(jnp.sum(tree_weights, axis=-1))
        rounded_cache = lax.optimization_barrier(cache_weights.astype(jnp.bfloat16)).astype(jnp.float32)
        rounded_tree = lax.optimization_barrier(tree_weights.astype(jnp.bfloat16)).astype(jnp.float32)
        numerator = jnp.einsum('nkgp,pkd->nkgd', rounded_cache, cvalue_one.astype(jnp.float32), precision=lax.Precision.HIGHEST)
        numerator = numerator + jnp.einsum('nkgj,jkd->nkgd', rounded_tree, tvalue_one.astype(jnp.float32), precision=lax.Precision.HIGHEST)
        return (numerator / denominator[..., None]).astype(jnp.bfloat16).reshape(NODES, HEADS * HD)
    attended = lax.map(one_request, (query_grid, tree_key_grid, tree_value_grid, cache_key_grid, cache_value_grid, cache_lens, ancestor))
    attended = attended.reshape(REQUESTS * NODES, HEADS * HD)
    projected = jnp.dot(attended, out_weight, preferred_element_type=jnp.float32)
    tree_hidden = (residual.astype(jnp.float32) + projected).astype(jnp.bfloat16)
    picked_rows = (jnp.arange(REQUESTS, dtype=jnp.int32)[:, None] * NODES + accepted_nodes).reshape(-1)
    accepted_hidden = jnp.take(tree_hidden, picked_rows, axis=0)
    return (tree_hidden, accepted_hidden)
```

```python
import functools
import math

import jax
import jax.numpy as jnp
from jax import lax
from jax.experimental import pallas as pl
from jax.experimental.pallas import tpu as pltpu
from jax.sharding import PartitionSpec as P

HEADS = 64
KV_HEADS = 8
HD = 128
GROUP = HEADS // KV_HEADS
Z, Y, X, C = 8, 4, 4, 2
KEY_BLOCK = 512
neg_large = -1e30


def attention_kernel(
    lens_ref, parents_ref, q_ref, tk_ref, tv_ref, k_ref, v_ref, out_ref, scores, maxes
):
    request = pl.program_id(0)
    nodes = q_ref.shape[0]
    rows = nodes * GROUP
    scale = 1.0 / math.sqrt(HD)
    length = lens_ref[request]

    parents = parents_ref[0]
    col = lax.broadcasted_iota(jnp.int32, (nodes, nodes), 1)
    row = lax.broadcasted_iota(jnp.int32, (nodes, nodes), 0)
    reached = ((parents == col) | (row == col)).astype(jnp.bfloat16)
    for _ in range((nodes - 1).bit_length()):
        squared = jnp.dot(reached, reached, preferred_element_type=jnp.float32)
        reached = jnp.minimum(squared, 1.0).astype(jnp.bfloat16)
    ancestor = reached.astype(jnp.float32) > 0.5

    queries = jnp.concatenate([q_ref[:, g * HD : (g + 1) * HD] for g in range(GROUP)], axis=0)
    dims = (((1,), (1,)), ((), ()))
    tree = lax.dot_general(queries, tk_ref[...], dims, preferred_element_type=jnp.float32) * scale
    tree = jnp.where(jnp.concatenate([ancestor] * GROUP, axis=0), tree, neg_large)
    maxes[...] = jnp.full(maxes.shape, neg_large, jnp.float32)
    blocks = (length + KEY_BLOCK - 1) // KEY_BLOCK

    def score(b, carry):
        start = pl.multiple_of(b * KEY_BLOCK, KEY_BLOCK)
        s = lax.dot_general(
            queries, k_ref[0, pl.ds(start, KEY_BLOCK), :], dims, preferred_element_type=jnp.float32
        )
        pos = start + lax.broadcasted_iota(jnp.int32, (1, KEY_BLOCK), 1)
        s = jnp.where(pos < length, s * scale, neg_large)
        scores[b] = s
        top = maxes[...]
        for i in range(KEY_BLOCK // HD):
            top = jnp.maximum(top, s[:, i * HD : (i + 1) * HD])
        maxes[...] = top
        return carry

    lax.fori_loop(0, blocks, score, 0)
    row_max = jnp.maximum(
        jnp.max(maxes[...], axis=1, keepdims=True), jnp.max(tree, axis=1, keepdims=True)
    )
    tree_weights = jnp.exp(tree - row_max)
    total = jnp.sum(tree_weights, axis=1, keepdims=True)
    acc = jnp.dot(
        tree_weights.astype(jnp.bfloat16), tv_ref[...], preferred_element_type=jnp.float32
    )

    def absorb(b, carry):
        acc, sums = carry
        start = pl.multiple_of(b * KEY_BLOCK, KEY_BLOCK)
        w = jnp.exp(scores[b] - row_max)
        for i in range(KEY_BLOCK // HD):
            sums = sums + w[:, i * HD : (i + 1) * HD]
        acc = acc + jnp.dot(
            w.astype(jnp.bfloat16),
            v_ref[0, pl.ds(start, KEY_BLOCK), :],
            preferred_element_type=jnp.float32,
        )
        return acc, sums

    acc, sums = lax.fori_loop(0, blocks, absorb, (acc, jnp.zeros((rows, HD), jnp.float32)))
    total = total + jnp.sum(sums, axis=1, keepdims=True)
    attended = (acc / total).astype(out_ref.dtype)
    for g in range(GROUP):
        out_ref[:, g * HD : (g + 1) * HD] = attended[g * nodes : (g + 1) * nodes]


def attention(queries, tree_keys, tree_values, cache_keys, cache_values, cache_lens, parents):
    requests, nodes = parents.shape
    cache = cache_keys.shape[1]
    rows = nodes * GROUP
    per_node = lambda width: pl.BlockSpec((nodes, width), lambda r, lens: (r, 0))
    per_cache = pl.BlockSpec((1, cache, HD), lambda r, lens: (r, 0, 0))
    return pl.pallas_call(
        attention_kernel,
        grid_spec=pltpu.PrefetchScalarGridSpec(
            num_scalar_prefetch=1,
            grid=(requests,),
            in_specs=[
                pl.BlockSpec((1, nodes, 1), lambda r, lens: (r, 0, 0)),
                per_node(GROUP * HD),
                per_node(HD),
                per_node(HD),
                per_cache,
                per_cache,
            ],
            out_specs=per_node(GROUP * HD),
            scratch_shapes=[
                pltpu.VMEM((cache // KEY_BLOCK, rows, KEY_BLOCK), jnp.float32),
                pltpu.VMEM((rows, HD), jnp.float32),
            ],
        ),
        out_shape=jax.ShapeDtypeStruct(queries.shape, jnp.bfloat16),
        compiler_params=pltpu.CompilerParams(vmem_limit_bytes=40 * 1024 * 1024),
        cost_estimate=pl.CostEstimate(
            flops=requests * rows * cache * HD * 8,
            bytes_accessed=requests * cache * HD * 4,
            transcendentals=requests * rows * cache,
        ),
        name="attention",
    )(cache_lens, parents[:, :, None], queries, tree_keys, tree_values, cache_keys, cache_values)


def shift_z(value, by):
    pairs = [(z * Y + y, (z + by) % Z * Y + y) for z in range(Z) for y in range(Y)]
    return lax.ppermute(value, "dp", pairs)


def shift_y(value, by):
    pairs = [(z * Y + y, z * Y + (y + by) % Y) for z in range(Z) for y in range(Y)]
    return lax.ppermute(value, "dp", pairs)


def shift_x(value, by):
    pairs = [(x * C + c, (x + by) % X * C + c) for x in range(X) for c in range(C)]
    return lax.ppermute(value, "mp", pairs)


def swap_core(value):
    return lax.ppermute(value, "mp", [(j, j ^ 1) for j in range(X * C)])


def per_device(
    queries,
    tree_keys,
    tree_values,
    cache_keys,
    cache_values,
    cache_lens,
    parents,
    accepted_nodes,
    residual,
    out_weight,
):
    dp, mp = lax.axis_index("dp"), lax.axis_index("mp")
    z, y, x, c = dp // Y, dp % Y, mp // C, mp % C
    requests, nodes = parents.shape
    accepted = accepted_nodes.shape[1]
    rows = requests * nodes
    inner, width = out_weight.shape
    f32, bf16 = jnp.float32, jnp.bfloat16

    weights = [out_weight] + [None] * (Z - 1)
    ahead = behind = out_weight
    for d in range(1, Z // 2):
        ahead, behind = shift_z(ahead, -1), shift_z(behind, 1)
        weights[d], weights[Z - d] = ahead, behind
    half = inner // 2
    weights[Z // 2] = jnp.concatenate(
        [shift_z(ahead[:half], -1), shift_z(behind[half:], 1)], axis=0
    )

    def my_columns(owner):
        return lax.dynamic_slice_in_dim(residual, owner * width, width, 1)

    node_rows = (jnp.arange(requests, dtype=jnp.int32)[:, None] * nodes + accepted_nodes).reshape(-1)
    residuals = [my_columns(y)] + [shift_y(my_columns((y + q) % Y), q) for q in range(1, Y)]
    picked = [node_rows] + [shift_y(node_rows, q) for q in range(1, Y)]

    attended = attention(
        queries, tree_keys, tree_values, cache_keys, cache_values, cache_lens, parents
    )
    gathered = jnp.concatenate([attended] + [shift_y(attended, q) for q in range(1, Y)], axis=0)

    partial = [jnp.dot(gathered, w, preferred_element_type=f32) for w in weights]
    odd = (z + c) % 2
    kept = [jnp.where(odd == 0, partial[2 * e], partial[2 * e + 1]) for e in range(X)]
    given = [jnp.where(odd == 0, partial[2 * e + 1], partial[2 * e]).astype(bf16) for e in range(X)]
    come = swap_core(jnp.stack(given))
    summed = jnp.stack([k + come[e].astype(f32) for e, k in enumerate(kept)])
    base = (z + odd) // 2

    def block_for(chip):
        return lax.dynamic_index_in_dim(summed, (chip - base) % X, 0, keepdims=False)

    own = block_for(x)
    for by in range(1, X):
        own = own + shift_x(block_for((x + by) % X).astype(bf16), by).astype(f32)
    final = (jnp.concatenate(residuals, axis=0).astype(f32) + own).astype(bf16)

    home = [final[:rows]] + [shift_y(final[q * rows : (q + 1) * rows], -q) for q in range(1, Y)]
    columns = jnp.stack(home)
    columns = lax.dynamic_slice_in_dim(jnp.concatenate([columns, columns]), (Y - y) % Y, Y, 0)
    tree_hidden = jnp.moveaxis(columns, 0, 1).reshape(rows, Y * width)

    wanted = jnp.concatenate([q * rows + picked[q] for q in range(Y)])
    tile = jnp.take(final, wanted, axis=0)
    count = requests * accepted
    everyone = lax.all_to_all(
        jnp.broadcast_to(tile[None], (Z * Y, *tile.shape)), "dp", 0, 0, tiled=True
    ).reshape(Z, Y, Y, count, width)
    accepted_hidden = jnp.stack(
        [
            jnp.stack([everyone[:, s, (s - owner) % Y] for s in range(Y)], axis=2)
            for owner in range(Y)
        ],
        axis=1,
    ).reshape(Z * Y * count, Y * width)
    return (tree_hidden, accepted_hidden)


def solution(mesh):
    placed = (
        P("dp", "mp"),
        P("dp", "mp"),
        P("dp", "mp"),
        P("dp", None, "mp"),
        P("dp", None, "mp"),
        P("dp"),
        P("dp", None),
        P("dp", None),
        P("dp", "mp"),
        P("mp", "dp"),
    )
    return jax.shard_map(
        per_device,
        mesh=mesh,
        in_specs=placed,
        out_specs=(P("dp", "mp"), P(None, "mp")),
        check_vma=False,
    )
```

```python
import math

import jax
import jax.numpy as jnp
from jax import lax
from jax.experimental import pallas as pl
from jax.experimental.pallas import tpu as pltpu
from jax.sharding import PartitionSpec as P

HEADS = 64
KV_HEADS = 8
HD = 128
GROUP = HEADS // KV_HEADS
Z, Y, X, C = 8, 4, 4, 2
KEY_BLOCK = 512
neg_large = -1e30


def attention_kernel(
    lens_ref, parents_ref, q_ref, tk_ref, tv_ref, k_ref, v_ref, out_ref, scores, maxes
):
    request = pl.program_id(0)
    nodes = q_ref.shape[0]
    rows = nodes * GROUP
    scale = 1.0 / math.sqrt(HD)
    length = lens_ref[request]

    parents = parents_ref[0]
    col = lax.broadcasted_iota(jnp.int32, (nodes, nodes), 1)
    row = lax.broadcasted_iota(jnp.int32, (nodes, nodes), 0)
    reached = ((parents == col) | (row == col)).astype(jnp.bfloat16)
    for _ in range((nodes - 1).bit_length()):
        squared = jnp.dot(reached, reached, preferred_element_type=jnp.float32)
        reached = jnp.minimum(squared, 1.0).astype(jnp.bfloat16)
    ancestor = reached.astype(jnp.float32) > 0.5

    queries = jnp.concatenate([q_ref[:, g * HD : (g + 1) * HD] for g in range(GROUP)], axis=0)
    dims = (((1,), (1,)), ((), ()))
    tree = lax.dot_general(queries, tk_ref[...], dims, preferred_element_type=jnp.float32) * scale
    tree = jnp.where(jnp.concatenate([ancestor] * GROUP, axis=0), tree, neg_large)
    maxes[...] = jnp.full(maxes.shape, neg_large, jnp.float32)
    blocks = (length + KEY_BLOCK - 1) // KEY_BLOCK

    def score(b, carry):
        start = pl.multiple_of(b * KEY_BLOCK, KEY_BLOCK)
        s = lax.dot_general(
            queries, k_ref[0, pl.ds(start, KEY_BLOCK), :], dims, preferred_element_type=jnp.float32
        )
        pos = start + lax.broadcasted_iota(jnp.int32, (1, KEY_BLOCK), 1)
        s = jnp.where(pos < length, s * scale, neg_large)
        scores[b] = s
        top = maxes[...]
        for i in range(KEY_BLOCK // HD):
            top = jnp.maximum(top, s[:, i * HD : (i + 1) * HD])
        maxes[...] = top
        return carry

    lax.fori_loop(0, blocks, score, 0)
    row_max = jnp.maximum(
        jnp.max(maxes[...], axis=1, keepdims=True), jnp.max(tree, axis=1, keepdims=True)
    )
    tree_weights = jnp.exp(tree - row_max)
    total = jnp.sum(tree_weights, axis=1, keepdims=True)
    acc = jnp.dot(
        tree_weights.astype(jnp.bfloat16), tv_ref[...], preferred_element_type=jnp.float32
    )

    def absorb(b, carry):
        acc, sums = carry
        start = pl.multiple_of(b * KEY_BLOCK, KEY_BLOCK)
        w = jnp.exp(scores[b] - row_max)
        for i in range(KEY_BLOCK // HD):
            sums = sums + w[:, i * HD : (i + 1) * HD]
        acc = acc + jnp.dot(
            w.astype(jnp.bfloat16),
            v_ref[0, pl.ds(start, KEY_BLOCK), :],
            preferred_element_type=jnp.float32,
        )
        return acc, sums

    acc, sums = lax.fori_loop(0, blocks, absorb, (acc, jnp.zeros((rows, HD), jnp.float32)))
    total = total + jnp.sum(sums, axis=1, keepdims=True)
    attended = (acc / total).astype(out_ref.dtype)
    for g in range(GROUP):
        out_ref[:, g * HD : (g + 1) * HD] = attended[g * nodes : (g + 1) * nodes]


def attention(queries, tree_keys, tree_values, cache_keys, cache_values, cache_lens, parents):
    requests, nodes = parents.shape
    cache = cache_keys.shape[1]
    rows = nodes * GROUP
    per_node = lambda width: pl.BlockSpec((nodes, width), lambda r, lens: (r, 0))
    per_cache = pl.BlockSpec((1, cache, HD), lambda r, lens: (r, 0, 0))
    return pl.pallas_call(
        attention_kernel,
        grid_spec=pltpu.PrefetchScalarGridSpec(
            num_scalar_prefetch=1,
            grid=(requests,),
            in_specs=[
                pl.BlockSpec((1, nodes, 1), lambda r, lens: (r, 0, 0)),
                per_node(GROUP * HD),
                per_node(HD),
                per_node(HD),
                per_cache,
                per_cache,
            ],
            out_specs=per_node(GROUP * HD),
            scratch_shapes=[
                pltpu.VMEM((cache // KEY_BLOCK, rows, KEY_BLOCK), jnp.float32),
                pltpu.VMEM((rows, HD), jnp.float32),
            ],
        ),
        out_shape=jax.ShapeDtypeStruct(queries.shape, jnp.bfloat16),
        compiler_params=pltpu.CompilerParams(vmem_limit_bytes=62 * 1024 * 1024),
        cost_estimate=pl.CostEstimate(
            flops=requests * rows * cache * HD * 8,
            bytes_accessed=requests * cache * HD * 4,
            transcendentals=requests * rows * cache,
        ),
        name="attention",
    )(cache_lens, parents[:, :, None], queries, tree_keys, tree_values, cache_keys, cache_values)


def home_kernel(place_ref, residual_ref, *refs):
    pieces, out_ref = refs[:Y], refs[Y]
    width = pieces[0].shape[1]
    for q, piece in enumerate(pieces):
        columns = pl.ds(pl.multiple_of(place_ref[q] * width, width), width)
        out_ref[:, columns] = (
            residual_ref[:, columns].astype(jnp.float32) + piece[...].astype(jnp.float32)
        ).astype(out_ref.dtype)


def add_at_home(residual, pieces, places):
    return pl.pallas_call(
        home_kernel,
        in_specs=[pl.BlockSpec(memory_space=pltpu.SMEM)]
        + [pl.BlockSpec(memory_space=pltpu.VMEM)] * (1 + Y),
        out_specs=pl.BlockSpec(memory_space=pltpu.VMEM),
        out_shape=jax.ShapeDtypeStruct(residual.shape, residual.dtype),
        cost_estimate=pl.CostEstimate(
            flops=residual.size, bytes_accessed=residual.size * 6, transcendentals=0
        ),
        name="home",
    )(places, residual, *pieces)


def owner_kernel(want_ref, come_ref, *refs):
    blocks, outs = refs[:Z], refs[Z:]
    for r, out in enumerate(outs):
        for d, block in enumerate(blocks):

            @pl.when(want_ref[r] == d)
            def _():
                out[...] = (
                    block[...].astype(jnp.float32) + come_ref[d // 2].astype(jnp.float32)
                ).astype(out.dtype)


def owner_sums(blocks, come, want):
    shape = blocks[0].shape
    return pl.pallas_call(
        owner_kernel,
        in_specs=[pl.BlockSpec(memory_space=pltpu.SMEM)]
        + [pl.BlockSpec(memory_space=pltpu.VMEM)] * (1 + Z),
        out_specs=[pl.BlockSpec(memory_space=pltpu.VMEM)] * X,
        out_shape=[jax.ShapeDtypeStruct(shape, jnp.float32)]
        + [jax.ShapeDtypeStruct(shape, jnp.bfloat16)] * (X - 1),
        cost_estimate=pl.CostEstimate(
            flops=blocks[0].size * X, bytes_accessed=blocks[0].size * 24, transcendentals=0
        ),
        name="owner_sums",
    )(want, come, *blocks)


def place_kernel(at_ref, *refs):
    parts, out_ref = refs[:Y], refs[Y]
    for r in range(Z):
        for q, part in enumerate(parts):
            out_ref[(at_ref[0] + Z - r) % Z, (at_ref[1] + Y - q) % Y] = part[r]


def place_accepted(parts, at):
    _, count, width = parts[0].shape
    return pl.pallas_call(
        place_kernel,
        in_specs=[pl.BlockSpec(memory_space=pltpu.SMEM)]
        + [pl.BlockSpec(memory_space=pltpu.VMEM)] * Y,
        out_specs=pl.BlockSpec(memory_space=pltpu.VMEM),
        out_shape=jax.ShapeDtypeStruct((Z, Y, count, width), parts[0].dtype),
        cost_estimate=pl.CostEstimate(
            flops=parts[0].size, bytes_accessed=parts[0].size * 16, transcendentals=0
        ),
        name="place_accepted",
    )(at, *parts)


def device(z, y, j):
    return (z * Y + y) * X * C + j


def shift_z(value, by):
    pairs = [(z * Y + y, (z + by) % Z * Y + y) for z in range(Z) for y in range(Y)]
    return lax.ppermute(value, "dp", pairs)


def shift_y(value, by):
    pairs = [(z * Y + y, z * Y + (y + by) % Y) for z in range(Z) for y in range(Y)]
    return lax.ppermute(value, "dp", pairs)


def shift_x(value, by):
    pairs = [(x * C + c, (x + by) % X * C + c) for x in range(X) for c in range(C)]
    return lax.ppermute(value, "mp", pairs)


def swap_core(value):
    return lax.ppermute(value, "mp", [(j, j ^ 1) for j in range(X * C)])


def per_device(
    queries,
    tree_keys,
    tree_values,
    cache_keys,
    cache_values,
    cache_lens,
    parents,
    accepted_nodes,
    residual,
    out_weight,
):
    dp, mp = lax.axis_index("dp"), lax.axis_index("mp")
    z, y, x, c = dp // Y, dp % Y, mp // C, mp % C
    requests, nodes = parents.shape
    accepted = accepted_nodes.shape[1]
    rows = requests * nodes
    count = requests * accepted
    inner, width = out_weight.shape
    f32, bf16 = jnp.float32, jnp.bfloat16

    weights = [out_weight] + [None] * (Z - 1)
    ahead = behind = out_weight
    for d in range(1, Z // 2):
        ahead, behind = shift_z(ahead, -1), shift_z(behind, 1)
        weights[d], weights[Z - d] = ahead, behind
    half = inner // 2
    low, high = shift_z(ahead[:half], -1), shift_z(behind[half:], 1)
    across = [out_weight] + [shift_y(out_weight, q) for q in range(1, Y)]

    attended = attention(
        queries, tree_keys, tree_values, cache_keys, cache_values, cache_lens, parents
    )
    node_rows = (jnp.arange(requests, dtype=jnp.int32)[:, None] * nodes + accepted_nodes).reshape(-1)
    gathered = [attended] + [shift_y(attended, q) for q in range(1, Y)]

    picked = jnp.take(attended, node_rows, axis=0)
    picked = [picked] + [shift_z(picked, r) for r in range(1, Z)]
    picked = jnp.concatenate(picked, axis=0)
    picked_part = jnp.concatenate(
        [jnp.dot(picked, w, preferred_element_type=f32).astype(bf16) for w in across], axis=1
    )
    picked_sum = lax.all_to_all(picked_part.reshape(Z, count, Y * width), "mp", 0, 0, tiled=True)
    picked_sum = picked_sum.astype(f32).sum(axis=0).astype(bf16)
    pairs = [
        (device(zz, yy, j), device((zz - j) % Z, yy, zz))
        for zz in range(Z)
        for yy in range(Y)
        for j in range(X * C)
    ]
    picked_sum = lax.ppermute(picked_sum, ("dp", "mp"), pairs)
    tile = add_at_home(
        jnp.take(residual, node_rows, axis=0),
        [picked_sum[:, q * width : (q + 1) * width] for q in range(Y)],
        (y - jnp.arange(Y)) % Y,
    )
    tiles = jnp.stack([tile] + [shift_z(tile, r) for r in range(1, Z)])
    parts = [tiles] + [shift_y(tiles, q) for q in range(1, Y)]
    accepted_hidden = place_accepted(parts, jnp.stack([z, y])).reshape(Z * Y * count, Y * width)

    gathered = jnp.concatenate(gathered, axis=0)
    partial = [
        jnp.dot(gathered, w, preferred_element_type=f32).astype(bf16) if d != Z // 2 else None
        for d, w in enumerate(weights)
    ]
    partial[Z // 2] = (
        jnp.dot(gathered[:, :half], low, preferred_element_type=f32)
        + jnp.dot(gathered[:, half:], high, preferred_element_type=f32)
    ).astype(bf16)
    odd = (z + c) % 2
    come = swap_core(
        jnp.stack([jnp.where(odd == 0, partial[2 * e + 1], partial[2 * e]) for e in range(X)]),
    )
    want = (x + jnp.arange(X) - (z + odd) // 2) % X * 2 + odd
    own, *sent = owner_sums(partial, come, want)
    for by in range(1, X):
        own = own + shift_x(sent[by - 1], by).astype(f32)
    own = own.astype(bf16)
    home = [own[:rows]] + [shift_y(own[q * rows : (q + 1) * rows], -q) for q in range(1, Y)]
    tree_hidden = add_at_home(residual, home, (y + jnp.arange(Y)) % Y)
    return (tree_hidden, accepted_hidden)


def solution(mesh):
    placed = (
        P("dp", "mp"),
        P("dp", "mp"),
        P("dp", "mp"),
        P("dp", None, "mp"),
        P("dp", None, "mp"),
        P("dp"),
        P("dp", None),
        P("dp", None),
        P("dp", "mp"),
        P("mp", "dp"),
    )

    return jax.shard_map(
        per_device,
        mesh=mesh,
        in_specs=placed,
        out_specs=(P("dp", "mp"), P(None, "mp")),
        check_vma=False,
    )
```

```python
import functools
import math

import jax
import jax.numpy as jnp
from jax import lax
from jax.experimental import pallas as pl
from jax.experimental.pallas import tpu as pltpu
from jax.sharding import PartitionSpec as P

HEADS = 64
KV_HEADS = 8
HD = 128
GROUP = HEADS // KV_HEADS
Z, Y, X, C = 8, 4, 4, 2
KEY_BLOCK = 512
neg_large = -1e30


def attention_kernel(
    lens_ref,
    parents_ref,
    q_ref,
    tk_ref,
    tv_ref,
    k_ref,
    v_ref,
    *rest,
    request,
):
    out_ref, scores, maxes = rest[-3:]
    nodes = q_ref.shape[0]
    rows = nodes * GROUP
    scale = 1.0 / math.sqrt(HD)
    length = lens_ref[request]

    parents = parents_ref[request : request + 1, :]
    col = lax.broadcasted_iota(jnp.int32, (nodes, nodes), 1)
    row = lax.broadcasted_iota(jnp.int32, (nodes, nodes), 0)
    reached = ((parents == row) | (row == col)).astype(jnp.bfloat16)
    for _ in range((nodes - 1).bit_length()):
        squared = jnp.dot(reached, reached, preferred_element_type=jnp.float32)
        reached = jnp.minimum(squared, 1.0).astype(jnp.bfloat16)
    ancestor = reached.astype(jnp.float32).T > 0.5

    queries = jnp.concatenate([q_ref[:, g * HD : (g + 1) * HD] for g in range(GROUP)], axis=0)
    dims = (((1,), (1,)), ((), ()))
    tree = lax.dot_general(queries, tk_ref[...], dims, preferred_element_type=jnp.float32) * scale
    tree = jnp.where(jnp.concatenate([ancestor] * GROUP, axis=0), tree, neg_large)
    maxes[...] = jnp.full(maxes.shape, neg_large, jnp.float32)
    blocks = (length + KEY_BLOCK - 1) // KEY_BLOCK

    def score(b, carry):
        start = pl.multiple_of(b * KEY_BLOCK, KEY_BLOCK)
        s = lax.dot_general(
            queries, k_ref[0, pl.ds(start, KEY_BLOCK), :], dims, preferred_element_type=jnp.float32
        )
        pos = start + lax.broadcasted_iota(jnp.int32, (1, KEY_BLOCK), 1)
        s = jnp.where(pos < length, s * scale, neg_large)
        scores[b] = s
        top = maxes[...]
        for i in range(KEY_BLOCK // HD):
            top = jnp.maximum(top, s[:, i * HD : (i + 1) * HD])
        maxes[...] = top
        return carry

    lax.fori_loop(0, blocks, score, 0)
    row_max = jnp.maximum(
        jnp.max(maxes[...], axis=1, keepdims=True), jnp.max(tree, axis=1, keepdims=True)
    )
    tree_weights = jnp.exp(tree - row_max)
    total = jnp.sum(tree_weights, axis=1, keepdims=True)
    acc = jnp.dot(
        tree_weights.astype(jnp.bfloat16), tv_ref[...], preferred_element_type=jnp.float32
    )

    def absorb(b, carry):
        acc, sums = carry
        start = pl.multiple_of(b * KEY_BLOCK, KEY_BLOCK)
        w = jnp.exp(scores[b] - row_max)
        for i in range(KEY_BLOCK // HD):
            sums = sums + w[:, i * HD : (i + 1) * HD]
        acc = acc + jnp.dot(
            w.astype(jnp.bfloat16),
            v_ref[0, pl.ds(start, KEY_BLOCK), :],
            preferred_element_type=jnp.float32,
        )
        return acc, sums

    acc, sums = lax.fori_loop(0, blocks, absorb, (acc, jnp.zeros((rows, HD), jnp.float32)))
    total = total + jnp.sum(sums, axis=1, keepdims=True)
    attended = (acc / total).astype(out_ref.dtype)
    for g in range(GROUP):
        out_ref[:, g * HD : (g + 1) * HD] = attended[g * nodes : (g + 1) * nodes]


def attention(
    request, earlier, queries, tree_keys, tree_values, cache_keys, cache_values, cache_lens, parents
):
    _, nodes = parents.shape
    cache = cache_keys.shape[1]
    rows = nodes * GROUP
    per_node = lambda width: pl.BlockSpec((nodes, width), lambda i, lens: (request, 0))
    per_cache = pl.BlockSpec((1, cache, HD), lambda i, lens: (request, 0, 0))
    return pl.pallas_call(
        functools.partial(attention_kernel, request=request),
        grid_spec=pltpu.PrefetchScalarGridSpec(
            num_scalar_prefetch=1,
            grid=(1,),
            in_specs=[
                pl.BlockSpec(parents.shape, lambda i, lens: (0, 0)),
                per_node(GROUP * HD),
                per_node(HD),
                per_node(HD),
                per_cache,
                per_cache,
            ]
            + [pl.BlockSpec(memory_space=pl.ANY)] * len(earlier),
            out_specs=per_node(GROUP * HD),
            scratch_shapes=[
                pltpu.VMEM((cache // KEY_BLOCK, rows, KEY_BLOCK), jnp.float32),
                pltpu.VMEM((rows, HD), jnp.float32),
            ],
        ),
        out_shape=jax.ShapeDtypeStruct(queries.shape, jnp.bfloat16),
        input_output_aliases={7: 0} if earlier else {},
        compiler_params=pltpu.CompilerParams(vmem_limit_bytes=62 * 1024 * 1024),
        cost_estimate=pl.CostEstimate(
            flops=rows * cache * HD * 8,
            bytes_accessed=cache * HD * 4,
            transcendentals=rows * cache,
        ),
        name="attention",
    )(
        cache_lens,
        parents,
        queries,
        tree_keys,
        tree_values,
        cache_keys,
        cache_values,
        *earlier,
    )


def home_kernel(accepted_ref, residual_ref, parts_ref, out_ref, tile_ref):
    requests, count = accepted_ref.shape
    nodes = residual_ref.shape[0] // requests
    width = parts_ref.shape[2]
    for s in range(Y):
        columns = slice(s * width, (s + 1) * width)
        total = residual_ref[:, columns].astype(jnp.float32)
        for x in range(X):
            total = total + parts_ref[s * X + x].astype(jnp.float32)
        out_ref[:, columns] = total.astype(out_ref.dtype)
    for r in range(requests):
        hot = lax.broadcasted_iota(jnp.int32, (nodes, count), 0) == accepted_ref[r : r + 1, :]
        tile_ref[r * count : (r + 1) * count, :] = lax.dot_general(
            hot.astype(jnp.float32).astype(jnp.bfloat16),
            out_ref[r * nodes : (r + 1) * nodes, :],
            (((0,), (0,)), ((), ())),
            preferred_element_type=jnp.float32,
        ).astype(tile_ref.dtype)


def add_at_home(residual, parts, accepted_nodes):
    return pl.pallas_call(
        home_kernel,
        in_specs=[pl.BlockSpec(memory_space=pltpu.VMEM)] * 3,
        out_specs=[pl.BlockSpec(memory_space=pltpu.VMEM)] * 2,
        out_shape=[
            jax.ShapeDtypeStruct(residual.shape, residual.dtype),
            jax.ShapeDtypeStruct((accepted_nodes.size, residual.shape[1]), residual.dtype),
        ],
        cost_estimate=pl.CostEstimate(
            flops=residual.size * X, bytes_accessed=residual.size * 12, transcendentals=0
        ),
        name="home",
    )(accepted_nodes, residual, parts)


def owner_kernel(want_ref, y_ref, come_ref, *refs):
    blocks, out_ref = refs[:Z], refs[Z]
    rows = out_ref.shape[1]
    for chip in range(X):
        for d, block in enumerate(blocks):

            @pl.when(want_ref[chip] == d)
            def _():
                for q in range(Y):
                    part = slice(q * rows, (q + 1) * rows)
                    total = block[part].astype(jnp.float32) + come_ref[d // 2, part].astype(
                        jnp.float32
                    )
                    out_ref[(y_ref[0] + Y - q) % Y * X + chip] = total.astype(out_ref.dtype)


def owner_sums(blocks, come, want, y):
    rows, width = blocks[0].shape
    return pl.pallas_call(
        owner_kernel,
        in_specs=[pl.BlockSpec(memory_space=pltpu.SMEM)] * 2
        + [pl.BlockSpec(memory_space=pltpu.VMEM)] * (1 + Z),
        out_specs=pl.BlockSpec(memory_space=pltpu.VMEM),
        out_shape=jax.ShapeDtypeStruct((Y * X, rows // Y, width), jnp.bfloat16),
        cost_estimate=pl.CostEstimate(
            flops=blocks[0].size * X, bytes_accessed=blocks[0].size * 24, transcendentals=0
        ),
        name="owner_sums",
    )(want, y, come, *blocks)


def device(z, y, j):
    return (z * Y + y) * X * C + j


def shift_z(value, by):
    pairs = [(z * Y + y, (z + by) % Z * Y + y) for z in range(Z) for y in range(Y)]
    return lax.ppermute(value, "dp", pairs)


def shift_y(value, by):
    pairs = [(z * Y + y, z * Y + (y + by) % Y) for z in range(Z) for y in range(Y)]
    return lax.ppermute(value, "dp", pairs)


def swap_core(value):
    return lax.ppermute(value, "mp", [(j, j ^ 1) for j in range(X * C)])


def per_device(
    queries,
    tree_keys,
    tree_values,
    cache_keys,
    cache_values,
    cache_lens,
    parents,
    accepted_nodes,
    residual,
    out_weight,
):
    dp, mp = lax.axis_index("dp"), lax.axis_index("mp")
    z, y, c = dp // Y, dp % Y, mp % C
    requests, _ = parents.shape
    count = requests * accepted_nodes.shape[1]
    inner, width = out_weight.shape
    f32, bf16 = jnp.float32, jnp.bfloat16

    weights = [out_weight] + [None] * (Z - 1)
    ahead = behind = out_weight
    for d in range(1, Z // 2):
        ahead, behind = shift_z(ahead, -1), shift_z(behind, 1)
        weights[d], weights[Z - d] = ahead, behind
    half = inner // 2
    low, high = shift_z(ahead[:half], -1), shift_z(behind[half:], 1)

    attended = ()
    for r in range(requests):
        attended = attention(
            r,
            attended,
            queries,
            tree_keys,
            tree_values,
            cache_keys,
            cache_values,
            cache_lens,
            parents,
        )
        attended = (attended,)
    (attended,) = attended
    gathered = [attended] + [shift_y(attended, q) for q in range(1, Y)]

    gathered = jnp.concatenate(gathered, axis=0)
    partial = []
    for d, w in enumerate(weights):
        if d != Z // 2:
            total = jnp.dot(gathered, w, preferred_element_type=f32)
        else:
            total = jnp.dot(gathered[:, :half], low, preferred_element_type=f32)
            total = total + jnp.dot(gathered[:, half:], high, preferred_element_type=f32)
        partial.append(total.astype(bf16))
    odd = (z + c) % 2
    come = swap_core(
        jnp.stack([jnp.where(odd == 0, partial[2 * e + 1], partial[2 * e]) for e in range(X)]),
    )
    want = (jnp.arange(X) - (z + odd) // 2) % X * 2 + odd
    sums = owner_sums(partial, come, want, y[None])
    planes = [
        [device(zz, yy, xx * C + cc) for yy in range(Y) for xx in range(X)]
        for zz in range(Z)
        for cc in range(C)
    ]
    sums = lax.all_to_all(
        sums, ("dp", "mp"), 0, 0, axis_index_groups=planes, tiled=True
    )
    tree_hidden, tile = add_at_home(residual, sums, accepted_nodes)
    accepted_hidden = lax.all_to_all(
        jnp.broadcast_to(tile[None], (Z * Y, *tile.shape)), "dp", 0, 0, tiled=True
    ).reshape(Z * Y * count, Y * width)
    return (tree_hidden, accepted_hidden)


def solution(mesh):
    placed = (
        P("dp", "mp"),
        P("dp", "mp"),
        P("dp", "mp"),
        P("dp", None, "mp"),
        P("dp", None, "mp"),
        P("dp"),
        P("dp", None),
        P("dp", None),
        P("dp", "mp"),
        P("mp", "dp"),
    )

    return jax.shard_map(
        per_device,
        mesh=mesh,
        in_specs=placed,
        out_specs=(P("dp", "mp"), P(None, "mp")),
        check_vma=False,
    )
```

```python
import functools
import math

import jax
import jax.numpy as jnp
from jax import lax
from jax.experimental import pallas as pl
from jax.experimental.pallas import tpu as pltpu
from jax.sharding import PartitionSpec as P

HEADS = 64
KV_HEADS = 8
HD = 128
GROUP = HEADS // KV_HEADS
NODES, ACC = 64, 8
Z, Y, X, C = 8, 4, 4, 2
KEY_BLOCK = 1024
neg_large = -1e30


def attention_kernel(
    lens_ref,
    parents_ref,
    q_ref,
    tk_ref,
    tv_ref,
    k_ref,
    v_ref,
    accepted_ref,
    *rest,
    request,
):
    out_ref, picked_ref, scores, acc = rest[-4:]
    nodes = q_ref.shape[0]
    rows = nodes * GROUP
    f32, bf16 = jnp.float32, jnp.bfloat16
    factor = math.log2(math.e) / math.sqrt(HD)
    length = lens_ref[request]

    row = lax.broadcasted_iota(jnp.int32, (nodes, nodes), 0)
    col = lax.broadcasted_iota(jnp.int32, (nodes, nodes), 1)
    parents = parents_ref[request : request + 1, :]
    reached = ((parents == row) | (row == col)).astype(f32).astype(bf16)
    for _ in range((nodes - 1).bit_length()):
        squared = jnp.dot(reached, reached, preferred_element_type=f32)
        reached = jnp.minimum(squared, 1.0).astype(bf16)
    head = lax.broadcasted_iota(jnp.int32, (nodes, rows), 1) % nodes
    repeat = head == lax.broadcasted_iota(jnp.int32, (nodes, rows), 0)
    ancestor = jnp.dot(reached, repeat.astype(f32).astype(bf16), preferred_element_type=f32) > 0.5

    queries = jnp.concatenate([q_ref[:, g * HD : (g + 1) * HD] for g in range(GROUP)], axis=0)
    last, first = (((1,), (1,)), ((), ())), (((0,), (0,)), ((), ()))
    tree = lax.dot_general(tk_ref[...], queries, last, preferred_element_type=f32) * factor
    tree = jnp.where(ancestor, tree, neg_large)
    blocks = (length + KEY_BLOCK - 1) // KEY_BLOCK

    def score(b, top):
        start = pl.multiple_of(b * KEY_BLOCK, KEY_BLOCK)
        keys = k_ref[0, pl.ds(start, KEY_BLOCK), :]
        s = lax.dot_general(keys, queries, last, preferred_element_type=f32) * factor
        position = start + lax.broadcasted_iota(jnp.int32, (KEY_BLOCK, 1), 0)
        s = jnp.where(position < length, s, neg_large)
        scores[b] = s
        return jnp.maximum(top, jnp.max(s, axis=0, keepdims=True))

    top = lax.fori_loop(0, blocks, score, jnp.max(tree, axis=0, keepdims=True))
    weights = jnp.exp2(tree - top)
    total = jnp.sum(weights, axis=0, keepdims=True)
    acc[...] = lax.dot_general(
        tv_ref[...], weights.astype(bf16), first, preferred_element_type=f32
    )

    def absorb(b, total):
        start = pl.multiple_of(b * KEY_BLOCK, KEY_BLOCK)
        w = jnp.exp2(scores[b] - top)
        acc[...] += lax.dot_general(
            v_ref[0, pl.ds(start, KEY_BLOCK), :],
            w.astype(bf16),
            first,
            preferred_element_type=f32,
        )
        return total + jnp.sum(w, axis=0, keepdims=True)

    total = lax.fori_loop(0, blocks, absorb, total)
    attended = (acc[...] / total).T.astype(out_ref.dtype)
    accepted = accepted_ref[request : request + 1, :]
    hot = lax.broadcasted_iota(jnp.int32, (nodes, accepted.shape[1]), 0) == accepted
    hot = hot.astype(f32).astype(bf16)
    for g in range(GROUP):
        one = attended[g * nodes : (g + 1) * nodes]
        out_ref[:, g * HD : (g + 1) * HD] = one
        picked_ref[:, g * HD : (g + 1) * HD] = lax.dot_general(
            hot, one, first, preferred_element_type=f32
        ).astype(picked_ref.dtype)


def attention(request, earlier, inputs):
    _, parents, queries, _, _, cache_keys, _, accepted_nodes = inputs
    nodes = parents.shape[1]
    cache = cache_keys.shape[1]
    rows = nodes * GROUP
    count = accepted_nodes.shape[1]
    width = queries.shape[1]
    per_node = lambda size: pl.BlockSpec((nodes, size), lambda i, lens: (request, 0))
    per_cache = pl.BlockSpec((1, cache, HD), lambda i, lens: (request, 0, 0))
    whole = lambda array: pl.BlockSpec(array.shape, lambda i, lens: (0, 0))
    return pl.pallas_call(
        functools.partial(attention_kernel, request=request),
        grid_spec=pltpu.PrefetchScalarGridSpec(
            num_scalar_prefetch=1,
            grid=(1,),
            in_specs=[
                whole(parents),
                per_node(width),
                per_node(HD),
                per_node(HD),
                per_cache,
                per_cache,
                whole(accepted_nodes),
            ]
            + [pl.BlockSpec(memory_space=pl.ANY)] * len(earlier),
            out_specs=[
                per_node(width),
                pl.BlockSpec((count, width), lambda i, lens: (0, 0)),
            ],
            scratch_shapes=[
                pltpu.VMEM((cache // KEY_BLOCK, KEY_BLOCK, rows), jnp.float32),
                pltpu.VMEM((HD, rows), jnp.float32),
            ],
        ),
        out_shape=[
            jax.ShapeDtypeStruct(queries.shape, jnp.bfloat16),
            jax.ShapeDtypeStruct((count, width), jnp.bfloat16),
        ],
        input_output_aliases={len(inputs): 0} if earlier else {},
        compiler_params=pltpu.CompilerParams(vmem_limit_bytes=62 * 1024 * 1024),
        cost_estimate=pl.CostEstimate(
            flops=rows * cache * HD * 8,
            bytes_accessed=cache * HD * 4,
            transcendentals=rows * cache,
        ),
        name="attention",
    )(*inputs, *earlier)


def home_kernel(place_ref, residual_ref, *refs):
    pieces, out_ref = refs[:Y], refs[Y]
    width = pieces[0].shape[1]
    for q, piece in enumerate(pieces):
        columns = pl.ds(pl.multiple_of(place_ref[q] * width, width), width)
        out_ref[:, columns] = (
            residual_ref[:, columns].astype(jnp.float32) + piece[...].astype(jnp.float32)
        ).astype(out_ref.dtype)


def in_columns(kernel, places, arrays, rows):
    return pl.pallas_call(
        kernel,
        in_specs=[pl.BlockSpec(memory_space=pltpu.SMEM)]
        + [pl.BlockSpec(memory_space=pltpu.VMEM)] * len(arrays),
        out_specs=pl.BlockSpec(memory_space=pltpu.VMEM),
        out_shape=jax.ShapeDtypeStruct((rows, Y * arrays[-1].shape[1]), jnp.bfloat16),
        cost_estimate=pl.CostEstimate(
            flops=rows * 1024, bytes_accessed=rows * 4096, transcendentals=0
        ),
    )(places, *arrays)


def owner_kernel(want_ref, come_ref, *refs):
    blocks, outs = refs[:Z], refs[Z:]
    for r, out in enumerate(outs):
        for d, block in enumerate(blocks):

            @pl.when(want_ref[r] == d)
            def _():
                out[...] = (
                    block[...].astype(jnp.float32) + come_ref[d // 2].astype(jnp.float32)
                ).astype(out.dtype)


def owner_sums(blocks, come, want):
    shape = come.shape[1:]
    first = pl.BlockSpec(shape, lambda i: (0, 0))
    return pl.pallas_call(
        owner_kernel,
        grid=(1,),
        in_specs=[pl.BlockSpec(memory_space=pltpu.SMEM)]
        + [pl.BlockSpec(come.shape, lambda i: (0, 0, 0))]
        + [first] * Z,
        out_specs=[first] * X,
        out_shape=[jax.ShapeDtypeStruct(shape, jnp.float32)]
        + [jax.ShapeDtypeStruct(shape, jnp.bfloat16)] * (X - 1),
        cost_estimate=pl.CostEstimate(
            flops=blocks[0].size * X, bytes_accessed=blocks[0].size * 24, transcendentals=0
        ),
        name="owner_sums",
    )(want, come, *blocks)


def gather_kernel(*refs):
    pieces, all_ref = refs[:Y], refs[Y]
    rows = NODES * pieces[0].shape[0] // (NODES + ACC)
    count = pieces[0].shape[0] - rows
    for q, piece in enumerate(pieces):
        all_ref[q * rows : (q + 1) * rows] = piece[:rows]
        all_ref[Y * rows + q * count : Y * rows + (q + 1) * count] = piece[rows:]


def gather_rows(pieces):
    size, width = pieces[0].shape
    return pl.pallas_call(
        gather_kernel,
        in_specs=[pl.BlockSpec(memory_space=pltpu.VMEM)] * Y,
        out_specs=pl.BlockSpec(memory_space=pltpu.VMEM),
        out_shape=jax.ShapeDtypeStruct((Y * size, width), jnp.bfloat16),
        cost_estimate=pl.CostEstimate(
            flops=Y * size * width, bytes_accessed=Y * size * width * 4, transcendentals=0
        ),
        name="gather_rows",
    )(*pieces)


def spread_kernel(at_ref, *refs):
    blocks, out_ref = refs[:Z], refs[Z]
    count = out_ref.shape[1]
    for d, block in enumerate(blocks):
        for q in range(Y):
            place = (at_ref[1] + Y - q) % Y * Z + (at_ref[0] + d) % Z
            out_ref[place] = block[q * count : (q + 1) * count, :]


def spread(blocks, at):
    size, width = blocks[0].shape
    few = size * ACC // (NODES + ACC)
    count = few // Y
    last = pl.BlockSpec((few, width), lambda i: (size // few - 1, 0))
    return pl.pallas_call(
        spread_kernel,
        grid=(1,),
        in_specs=[pl.BlockSpec(memory_space=pltpu.SMEM)] + [last] * Z,
        out_specs=pl.BlockSpec((Y * Z, count, width), lambda i: (0, 0, 0)),
        out_shape=jax.ShapeDtypeStruct((Y * Z, count, width), blocks[0].dtype),
        cost_estimate=pl.CostEstimate(
            flops=count * width, bytes_accessed=Z * Y * count * width * 4, transcendentals=0
        ),
        name="spread",
    )(at, *blocks)


def tile_kernel(accepted_ref, residual_ref, parts_ref, out_ref):
    requests, count = accepted_ref.shape
    nodes = residual_ref.shape[0] // requests
    width = parts_ref.shape[2]
    for r in range(requests):
        hot = lax.broadcasted_iota(jnp.int32, (nodes, count), 0) == accepted_ref[r : r + 1, :]
        kept = lax.dot_general(
            hot.astype(jnp.float32).astype(jnp.bfloat16),
            residual_ref[r * nodes : (r + 1) * nodes, :],
            (((0,), (0,)), ((), ())),
            preferred_element_type=jnp.float32,
        )
        took = slice(r * count, (r + 1) * count)
        for s in range(Y):
            total = kept[:, s * width : (s + 1) * width]
            for j in range(Z):
                total = total + parts_ref[s * Z + j, took].astype(jnp.float32)
            for copy in range(out_ref.shape[0]):
                out_ref[copy, took, s * width : (s + 1) * width] = total.astype(out_ref.dtype)


def accepted_tile(residual, accepted_nodes, parts, copies):
    count, width = parts.shape[1:]
    return pl.pallas_call(
        tile_kernel,
        in_specs=[pl.BlockSpec(memory_space=pltpu.VMEM)] * 3,
        out_specs=pl.BlockSpec(memory_space=pltpu.VMEM),
        out_shape=jax.ShapeDtypeStruct((copies, count, Y * width), residual.dtype),
        cost_estimate=pl.CostEstimate(
            flops=residual.size * 64, bytes_accessed=residual.size * 10, transcendentals=0
        ),
        name="accepted_tile",
    )(accepted_nodes, residual, parts)


def device(z, y, j):
    return (z * Y + y) * X * C + j


def shift_z(value, by):
    pairs = [(z * Y + y, (z + by) % Z * Y + y) for z in range(Z) for y in range(Y)]
    return lax.ppermute(value, "dp", pairs)


def shift_y(value, by):
    pairs = [(z * Y + y, z * Y + (y + by) % Y) for z in range(Z) for y in range(Y)]
    return lax.ppermute(value, "dp", pairs)


def shift_x(value, by):
    pairs = [(x * C + c, (x + by) % X * C + c) for x in range(X) for c in range(C)]
    return lax.ppermute(value, "mp", pairs)


def swap_core(value):
    return lax.ppermute(value, "mp", [(j, j ^ 1) for j in range(X * C)])


def per_device(
    queries,
    tree_keys,
    tree_values,
    cache_keys,
    cache_values,
    cache_lens,
    parents,
    accepted_nodes,
    residual,
    out_weight,
):
    dp, mp = lax.axis_index("dp"), lax.axis_index("mp")
    z, y, x, c = dp // Y, dp % Y, mp // C, mp % C
    requests, nodes = parents.shape
    rows = requests * nodes
    count = requests * accepted_nodes.shape[1]
    inner, width = out_weight.shape
    f32, bf16 = jnp.float32, jnp.bfloat16

    weights = [out_weight] + [None] * (Z - 1)
    ahead = behind = out_weight
    for d in range(1, Z // 2):
        ahead, behind = shift_z(ahead, -1), shift_z(behind, 1)
        weights[d], weights[Z - d] = ahead, behind
    half = inner // 2
    low, high = shift_z(ahead[:half], -1), shift_z(behind[half:], 1)

    inputs = (
        cache_lens,
        parents,
        queries,
        tree_keys,
        tree_values,
        cache_keys,
        cache_values,
        accepted_nodes,
    )
    earlier, picks = (), []
    for r in range(requests):
        attended, picked = attention(r, earlier, inputs)
        earlier = (attended,)
        picks.append(picked)
    packed = jnp.concatenate([attended, *picks], axis=0)
    packed = [packed] + [shift_y(packed, q) for q in range(1, Y)]
    gathered = gather_rows(packed)

    def partial(value, d):
        if d != Z // 2:
            total = jnp.dot(value, weights[d], preferred_element_type=f32)
        else:
            total = jnp.dot(value[:, :half], low, preferred_element_type=f32)
            total = total + jnp.dot(value[:, half:], high, preferred_element_type=f32)
        return total.astype(bf16)

    blocks = []
    for d in range(Z):
        blocks.append(partial(gathered, d))
    few = spread(blocks, jnp.stack([z, y]))
    planes = [
        [device(zz, yy, j) for yy in range(Y) for j in range(X * C)] for zz in range(Z)
    ]
    few = lax.all_to_all(few, ("dp", "mp"), 0, 0, axis_index_groups=planes, tiled=True)
    tiles = accepted_tile(residual, accepted_nodes, few, Z * Y)
    accepted_hidden = lax.all_to_all(tiles, "dp", 0, 0, tiled=True)
    accepted_hidden = accepted_hidden.reshape(Z * Y * count, Y * width)

    odd = (z + c) % 2
    come = swap_core(
        jnp.stack(
            [
                jnp.where(odd == 0, blocks[2 * e + 1], blocks[2 * e])[: Y * rows]
                for e in range(X)
            ]
        ),
    )
    want = (x + jnp.arange(X) - (z + odd) // 2) % X * 2 + odd
    own, *sent = owner_sums(blocks, come, want)
    for by in range(1, X):
        own = own + shift_x(sent[by - 1], by).astype(f32)
    own = own.astype(bf16)
    home = [own[:rows]] + [shift_y(own[q * rows : (q + 1) * rows], -q) for q in range(1, Y)]
    places = (y + jnp.arange(Y)) % Y
    tree_hidden = in_columns(home_kernel, places, [residual] + home, rows)
    return (tree_hidden, accepted_hidden)


def solution(mesh):
    placed = (
        P("dp", "mp"),
        P("dp", "mp"),
        P("dp", "mp"),
        P("dp", None, "mp"),
        P("dp", None, "mp"),
        P("dp"),
        P("dp", None),
        P("dp", None),
        P("dp", "mp"),
        P("mp", "dp"),
    )

    return jax.shard_map(
        per_device,
        mesh=mesh,
        in_specs=placed,
        out_specs=(P("dp", "mp"), P(None, "mp")),
        check_vma=False,
    )
```

```python
import functools
import math

import jax
import jax.numpy as jnp
from jax import lax
from jax.experimental import pallas as pl
from jax.experimental.pallas import tpu as pltpu
from jax.sharding import PartitionSpec as P

HEADS = 64
KV_HEADS = 8
HD = 128
GROUP = HEADS // KV_HEADS
NODES, ACC = 64, 8
Z, Y, X, C = 8, 4, 4, 2
KEY_BLOCK = 2048
neg_large = -1e30


def attention_kernel(
    lens_ref,
    parents_ref,
    q_ref,
    tk_ref,
    tv_ref,
    k_ref,
    v_ref,
    accepted_ref,
    *rest,
    request,
):
    *earlier, out_ref, scores, acc = rest
    nodes = q_ref.shape[0]
    rows = nodes * GROUP
    f32, bf16 = jnp.float32, jnp.bfloat16
    factor = math.log2(math.e) / math.sqrt(HD)
    length = lens_ref[request]

    row = lax.broadcasted_iota(jnp.int32, (nodes, nodes), 0)
    col = lax.broadcasted_iota(jnp.int32, (nodes, nodes), 1)
    parents = parents_ref[request : request + 1, :]
    reached = ((parents == row) | (row == col)).astype(f32).astype(bf16)
    for _ in range((nodes - 1).bit_length()):
        squared = jnp.dot(reached, reached, preferred_element_type=f32)
        reached = jnp.minimum(squared, 1.0).astype(bf16)
    head = lax.broadcasted_iota(jnp.int32, (nodes, rows), 1) % nodes
    repeat = head == lax.broadcasted_iota(jnp.int32, (nodes, rows), 0)
    ancestor = jnp.dot(reached, repeat.astype(f32).astype(bf16), preferred_element_type=f32) > 0.5

    queries = jnp.concatenate([q_ref[:, g * HD : (g + 1) * HD] for g in range(GROUP)], axis=0)
    last, first = (((1,), (1,)), ((), ())), (((0,), (0,)), ((), ()))
    tree = lax.dot_general(tk_ref[...], queries, last, preferred_element_type=f32) * factor
    tree = jnp.where(ancestor, tree, neg_large)
    blocks = (length + KEY_BLOCK - 1) // KEY_BLOCK

    def score(b, top):
        start = pl.multiple_of(b * KEY_BLOCK, KEY_BLOCK)
        keys = k_ref[0, pl.ds(start, KEY_BLOCK), :]
        s = lax.dot_general(keys, queries, last, preferred_element_type=f32) * factor
        position = start + lax.broadcasted_iota(jnp.int32, (KEY_BLOCK, 1), 0)
        s = jnp.where(position < length, s, neg_large)
        scores[b] = s
        return jnp.maximum(top, jnp.max(s, axis=0, keepdims=True))

    top = lax.fori_loop(0, blocks, score, jnp.max(tree, axis=0, keepdims=True))
    weights = jnp.exp2(tree - top)
    total = jnp.sum(weights, axis=0, keepdims=True)
    acc[...] = lax.dot_general(
        tv_ref[...], weights.astype(bf16), first, preferred_element_type=f32
    )

    def absorb(b, total):
        start = pl.multiple_of(b * KEY_BLOCK, KEY_BLOCK)
        w = jnp.exp2(scores[b] - top)
        acc[...] += lax.dot_general(
            v_ref[0, pl.ds(start, KEY_BLOCK), :],
            w.astype(bf16),
            first,
            preferred_element_type=f32,
        )
        return total + jnp.sum(w, axis=0, keepdims=True)

    total = lax.fori_loop(0, blocks, absorb, total)
    attended = (acc[...] / total).T.astype(out_ref.dtype)
    accepted = accepted_ref[request : request + 1, :]
    hot = lax.broadcasted_iota(jnp.int32, (nodes, accepted.shape[1]), 0) == accepted
    hot = hot.astype(f32).astype(bf16)
    mine = slice(request * nodes, (request + 1) * nodes)
    start = out_ref.shape[0] // (nodes + accepted.shape[1]) * nodes
    start = start + request * accepted.shape[1]
    for past in earlier:
        out_ref[...] = past[...]
    for g in range(GROUP):
        one = attended[g * nodes : (g + 1) * nodes]
        columns = slice(g * HD, (g + 1) * HD)
        out_ref[mine, columns] = one
        out_ref[start : start + accepted.shape[1], columns] = lax.dot_general(
            hot, one, first, preferred_element_type=f32
        ).astype(out_ref.dtype)


def attention(request, earlier, inputs):
    _, parents, queries, _, _, cache_keys, _, accepted_nodes = inputs
    requests, nodes = parents.shape
    cache = cache_keys.shape[1]
    rows = nodes * GROUP
    width = queries.shape[1]
    packed = (requests * (nodes + accepted_nodes.shape[1]), width)
    per_node = lambda size: pl.BlockSpec((nodes, size), lambda i, lens: (request, 0))
    per_cache = pl.BlockSpec((1, cache, HD), lambda i, lens: (request, 0, 0))
    whole = lambda array: pl.BlockSpec(array.shape, lambda i, lens: (0, 0))
    return pl.pallas_call(
        functools.partial(attention_kernel, request=request),
        grid_spec=pltpu.PrefetchScalarGridSpec(
            num_scalar_prefetch=1,
            grid=(1,),
            in_specs=[
                whole(parents),
                per_node(width),
                per_node(HD),
                per_node(HD),
                per_cache,
                per_cache,
                whole(accepted_nodes),
            ]
            + [whole(array) for array in earlier],
            out_specs=pl.BlockSpec(packed, lambda i, lens: (0, 0)),
            scratch_shapes=[
                pltpu.VMEM((cache // KEY_BLOCK, KEY_BLOCK, rows), jnp.float32),
                pltpu.VMEM((HD, rows), jnp.float32),
            ],
        ),
        out_shape=jax.ShapeDtypeStruct(packed, jnp.bfloat16),
        compiler_params=pltpu.CompilerParams(vmem_limit_bytes=62 * 1024 * 1024),
        cost_estimate=pl.CostEstimate(
            flops=rows * cache * HD * 8,
            bytes_accessed=cache * HD * 4,
            transcendentals=rows * cache,
        ),
        name="attention",
    )(*inputs, *earlier)


def home_kernel(place_ref, residual_ref, *refs):
    pieces, out_ref = refs[:Y], refs[Y]
    width = pieces[0].shape[1]
    for q, piece in enumerate(pieces):
        columns = pl.ds(pl.multiple_of(place_ref[q] * width, width), width)
        out_ref[:, columns] = (
            residual_ref[:, columns].astype(jnp.float32) + piece[...].astype(jnp.float32)
        ).astype(out_ref.dtype)


def in_columns(kernel, places, arrays, rows):
    return pl.pallas_call(
        kernel,
        in_specs=[pl.BlockSpec(memory_space=pltpu.SMEM)]
        + [pl.BlockSpec(memory_space=pltpu.VMEM)] * len(arrays),
        out_specs=pl.BlockSpec(memory_space=pltpu.VMEM),
        out_shape=jax.ShapeDtypeStruct((rows, Y * arrays[-1].shape[1]), jnp.bfloat16),
        cost_estimate=pl.CostEstimate(
            flops=rows * 1024, bytes_accessed=rows * 4096, transcendentals=0
        ),
    )(places, *arrays)


def owner_kernel(want_ref, come_ref, *refs):
    blocks, outs = refs[:Z], refs[Z:]
    for r, out in enumerate(outs):
        for d, block in enumerate(blocks):

            @pl.when(want_ref[r] == d)
            def _():
                out[...] = (
                    block[...].astype(jnp.float32) + come_ref[d // 2].astype(jnp.float32)
                ).astype(out.dtype)


def owner_sums(blocks, come, want):
    shape = come.shape[1:]
    first = pl.BlockSpec(shape, lambda i: (0, 0))
    return pl.pallas_call(
        owner_kernel,
        grid=(1,),
        in_specs=[pl.BlockSpec(memory_space=pltpu.SMEM)]
        + [pl.BlockSpec(come.shape, lambda i: (0, 0, 0))]
        + [first] * Z,
        out_specs=[first] * X,
        out_shape=[jax.ShapeDtypeStruct(shape, jnp.float32)]
        + [jax.ShapeDtypeStruct(shape, jnp.bfloat16)] * (X - 1),
        cost_estimate=pl.CostEstimate(
            flops=blocks[0].size * X, bytes_accessed=blocks[0].size * 24, transcendentals=0
        ),
        name="owner_sums",
    )(want, come, *blocks)


def gather_kernel(*refs):
    pieces, all_ref = refs[:Y], refs[Y]
    rows = NODES * pieces[0].shape[0] // (NODES + ACC)
    count = pieces[0].shape[0] - rows
    for q, piece in enumerate(pieces):
        all_ref[q * rows : (q + 1) * rows] = piece[:rows]
        all_ref[Y * rows + q * count : Y * rows + (q + 1) * count] = piece[rows:]


def gather_rows(pieces):
    size, width = pieces[0].shape
    return pl.pallas_call(
        gather_kernel,
        in_specs=[pl.BlockSpec(memory_space=pltpu.VMEM)] * Y,
        out_specs=pl.BlockSpec(memory_space=pltpu.VMEM),
        out_shape=jax.ShapeDtypeStruct((Y * size, width), jnp.bfloat16),
        cost_estimate=pl.CostEstimate(
            flops=Y * size * width, bytes_accessed=Y * size * width * 4, transcendentals=0
        ),
        name="gather_rows",
    )(*pieces)


def spread_kernel(z_ref, y_ref, *refs):
    blocks, out_ref = refs[:Z], refs[Z]
    count = out_ref.shape[1]
    for d, block in enumerate(blocks):
        for q in range(Y):
            place = (y_ref[0] + Y - q) % Y * Z + (z_ref[0] + d) % Z
            out_ref[place] = block[q * count : (q + 1) * count, :]


def spread(blocks, z, y):
    size, width = blocks[0].shape
    few = size * ACC // (NODES + ACC)
    count = few // Y
    last = pl.BlockSpec((few, width), lambda i: (size // few - 1, 0))
    return pl.pallas_call(
        spread_kernel,
        grid=(1,),
        in_specs=[pl.BlockSpec(memory_space=pltpu.SMEM)] * 2 + [last] * Z,
        out_specs=pl.BlockSpec((Y * Z, count, width), lambda i: (0, 0, 0)),
        out_shape=jax.ShapeDtypeStruct((Y * Z, count, width), blocks[0].dtype),
        cost_estimate=pl.CostEstimate(
            flops=count * width, bytes_accessed=Z * Y * count * width * 4, transcendentals=0
        ),
        name="spread",
    )(z, y, *blocks)


def place_kernel(y_ref, *refs):
    parts, out_ref = refs[:Y], refs[Y]
    for q, part in enumerate(parts):
        for z in range(Z):
            out_ref[z, (y_ref[0] + Y - q) % Y] = part[z]


def place_accepted(parts, y):
    _, count, width = parts[0].shape
    return pl.pallas_call(
        place_kernel,
        in_specs=[pl.BlockSpec(memory_space=pltpu.SMEM)]
        + [pl.BlockSpec(memory_space=pltpu.VMEM)] * Y,
        out_specs=pl.BlockSpec(memory_space=pltpu.VMEM),
        out_shape=jax.ShapeDtypeStruct((Z, Y, count, width), parts[0].dtype),
        cost_estimate=pl.CostEstimate(
            flops=parts[0].size, bytes_accessed=parts[0].size * 16, transcendentals=0
        ),
        name="place_accepted",
    )(y, *parts)


def tile_kernel(accepted_ref, residual_ref, parts_ref, out_ref):
    requests, count = accepted_ref.shape
    nodes = residual_ref.shape[0] // requests
    width = parts_ref.shape[2]
    for r in range(requests):
        hot = lax.broadcasted_iota(jnp.int32, (nodes, count), 0) == accepted_ref[r : r + 1, :]
        kept = lax.dot_general(
            hot.astype(jnp.float32).astype(jnp.bfloat16),
            residual_ref[r * nodes : (r + 1) * nodes, :],
            (((0,), (0,)), ((), ())),
            preferred_element_type=jnp.float32,
        )
        took = slice(r * count, (r + 1) * count)
        for s in range(Y):
            total = kept[:, s * width : (s + 1) * width]
            for j in range(Z):
                total = total + parts_ref[s * Z + j, took].astype(jnp.float32)
            for copy in range(out_ref.shape[0]):
                out_ref[copy, took, s * width : (s + 1) * width] = total.astype(out_ref.dtype)


def accepted_tile(residual, accepted_nodes, parts, copies):
    count, width = parts.shape[1:]
    return pl.pallas_call(
        tile_kernel,
        in_specs=[pl.BlockSpec(memory_space=pltpu.VMEM)] * 3,
        out_specs=pl.BlockSpec(memory_space=pltpu.VMEM),
        out_shape=jax.ShapeDtypeStruct((copies, count, Y * width), residual.dtype),
        cost_estimate=pl.CostEstimate(
            flops=residual.size * 64, bytes_accessed=residual.size * 10, transcendentals=0
        ),
        name="accepted_tile",
    )(accepted_nodes, residual, parts)


def device(z, y, j):
    return (z * Y + y) * X * C + j


def shift_z(value, by):
    pairs = [(z * Y + y, (z + by) % Z * Y + y) for z in range(Z) for y in range(Y)]
    return lax.ppermute(value, "dp", pairs)


def shift_y(value, by):
    pairs = [(z * Y + y, z * Y + (y + by) % Y) for z in range(Z) for y in range(Y)]
    return lax.ppermute(value, "dp", pairs)


def shift_x(value, by):
    pairs = [(x * C + c, (x + by) % X * C + c) for x in range(X) for c in range(C)]
    return lax.ppermute(value, "mp", pairs)


def swap_core(value):
    return lax.ppermute(value, "mp", [(j, j ^ 1) for j in range(X * C)])


def per_device(
    queries,
    tree_keys,
    tree_values,
    cache_keys,
    cache_values,
    cache_lens,
    parents,
    accepted_nodes,
    residual,
    out_weight,
):
    dp, mp = lax.axis_index("dp"), lax.axis_index("mp")
    z, y, x, c = dp // Y, dp % Y, mp // C, mp % C
    requests, nodes = parents.shape
    rows = requests * nodes
    count = requests * accepted_nodes.shape[1]
    inner, width = out_weight.shape
    f32, bf16 = jnp.float32, jnp.bfloat16

    weights = [out_weight] + [None] * (Z - 1)
    ahead = behind = out_weight
    for d in range(1, Z // 2):
        ahead, behind = shift_z(ahead, -1), shift_z(behind, 1)
        weights[d], weights[Z - d] = ahead, behind
    half = inner // 2
    low, high = shift_z(ahead[:half], -1), shift_z(behind[half:], 1)

    inputs = (
        cache_lens,
        parents,
        queries,
        tree_keys,
        tree_values,
        cache_keys,
        cache_values,
        accepted_nodes,
    )
    earlier = ()
    for r in range(requests):
        packed = attention(r, earlier, inputs)
        earlier = (packed,)
    packed = [packed] + [shift_y(packed, q) for q in range(1, Y)]
    gathered = gather_rows(packed)

    def partial(value, d):
        if d != Z // 2:
            total = jnp.dot(value, weights[d], preferred_element_type=f32)
        else:
            total = jnp.dot(value[:, :half], low, preferred_element_type=f32)
            total = total + jnp.dot(value[:, half:], high, preferred_element_type=f32)
        return total.astype(bf16)

    blocks = []
    for d in range(Z):
        blocks.append(partial(gathered, d))
    few = spread(blocks, z[None], y[None])
    planes = [
        [device(zz, yy, j) for yy in range(Y) for j in range(X * C)] for zz in range(Z)
    ]
    few = lax.all_to_all(few, ("dp", "mp"), 0, 0, axis_index_groups=planes, tiled=True)
    tiles = accepted_tile(residual, accepted_nodes, few, Z)
    along_z = [[zz * Y + yy for zz in range(Z)] for yy in range(Y)]
    tiles = lax.all_to_all(tiles, "dp", 0, 0, axis_index_groups=along_z, tiled=True)
    tiles = [tiles] + [shift_y(tiles, q) for q in range(1, Y)]
    accepted_hidden = place_accepted(tiles, y[None]).reshape(Z * Y * count, Y * width)

    odd = (z + c) % 2
    come = swap_core(
        jnp.stack(
            [
                jnp.where(odd == 0, blocks[2 * e + 1], blocks[2 * e])[: Y * rows]
                for e in range(X)
            ]
        ),
    )
    want = (x + jnp.arange(X) - (z + odd) // 2) % X * 2 + odd
    own, *sent = owner_sums(blocks, come, want)
    for by in range(1, X):
        own = own + shift_x(sent[by - 1], by).astype(f32)
    own = own.astype(bf16)
    home = [own[:rows]] + [shift_y(own[q * rows : (q + 1) * rows], -q) for q in range(1, Y)]
    places = (y + jnp.arange(Y)) % Y
    tree_hidden = in_columns(home_kernel, places, [residual] + home, rows)
    return (tree_hidden, accepted_hidden)


def solution(mesh):
    placed = (
        P("dp", "mp"),
        P("dp", "mp"),
        P("dp", "mp"),
        P("dp", None, "mp"),
        P("dp", None, "mp"),
        P("dp"),
        P("dp", None),
        P("dp", None),
        P("dp", "mp"),
        P("mp", "dp"),
    )

    return jax.shard_map(
        per_device,
        mesh=mesh,
        in_specs=placed,
        out_specs=(P("dp", "mp"), P(None, "mp")),
        check_vma=False,
    )
```
